32 devices in a mesh: tok: 4 (over y, x), row: 2 (over core), col: 4 (over z).
Axes of the slice: x: 2, y: 2, z: 4, core: 2. Of those that a mesh axis runs over, the one named last changes fastest.
Arguments:
- activations: bfloat16 [2048, 4096], P(('tok', 'col'), 'row'), may hold values from -6 to 6
- grads_t: bfloat16 [4, 7392, 2048], P(None, 'col', ('tok', 'row')), may hold values from -0.14941406 to 0.14941406
Outputs:
- weight_grad: float32 [4, 7392, 4096], P('tok', 'col', 'row')
The draws below stay inside these ranges and needn't reach their ends.
All inputs are finite; a program needn't handle non-finite values.
Results may differ from the reference program's by a relative error of at most 0.0003.
Values may be sent and summed in bfloat16 or wider, within the bound.
A program may use at most 128 MiB of HBM per device.

```python
import jax
import jax.numpy as jnp

D = 4096
FF = 29568
TOK_DEV = 512
TOKENS = 2048
N_TOK = 4


def raised(drawn, stream_key, source, target, shards_of, factor):
    def block_of(dim):
        return (jnp.arange(drawn.shape[dim]) // (drawn.shape[dim] // shards_of)).reshape((-1,) + (1,) * (drawn.ndim - 1 - dim))

    first = jax.random.permutation(stream_key, shards_of)[block_of(target)]
    second = (block_of(target) + shards_of // 2) % shards_of
    return jnp.where((block_of(source) == first) | (block_of(source) == second), factor * drawn, drawn)


def shard_levels(stream_key, extent, split, low, high):
    def one(dim, shards_of):
        draws = jax.random.uniform(jax.random.fold_in(jax.random.fold_in(stream_key, 6), dim), (shards_of,), jnp.float32, low / len(split), high / len(split))
        return jnp.repeat(jnp.exp(draws), extent[dim] // shards_of).reshape((-1,) + (1,) * (len(extent) - dim - 1))

    level = one(*split[0])
    for cut in split[1:]:
        level = level * one(*cut)
    return level


def noise(rng, dims, spread, bound, split=(), kind=jnp.bfloat16):
    factor_of = shard_levels(rng, dims, split, -0.22, 0.18) if split else 1.0
    entries = jax.random.normal(rng, dims, jnp.float32) * spread * factor_of
    return jnp.minimum(jnp.maximum(entries, -bound), bound).astype(kind)


def gaussian_with(rng, dims, spread, reach, shards, heavy, held_as=jnp.bfloat16):
    values = spread * jax.random.normal(rng, dims, jnp.float32)
    if shards:
        values = values * shard_levels(rng, dims, shards, -0.22, 0.18)
    return jnp.clip(raised(values, jax.random.fold_in(rng, 3), *heavy), -reach, reach).astype(held_as)


def setup_inputs(seed: int = 0) -> dict:
    splits = jax.random.split(jax.random.key(seed), 3)
    return {
        "activations": noise(splits[0], (TOKENS, D), 1.0, 6.0, ((0, 16), (1, 2))),
        "grads_t": gaussian_with(splits[1], (N_TOK, FF // N_TOK, TOKENS), 0.025, 0.14941406, ((1, 4), (2, 8)), (2, 0, 4, 2.0)),
    }


def reference(activations, grads_t):
    flat = grads_t.reshape(FF, TOKENS)
    total = jnp.zeros((FF, D), jnp.float32)
    for group in range(N_TOK):
        block = flat[:, group * TOK_DEV:(group + 1) * TOK_DEV]
        rows = activations[group * TOK_DEV:(group + 1) * TOK_DEV]
        total = total + jnp.dot(block, rows, preferred_element_type=jnp.float32)
    return total.reshape(N_TOK, FF // N_TOK, D)
```

```python
import functools

import jax
import jax.numpy as jnp
from jax import lax
from jax.experimental import pallas as pl
from jax.experimental.pallas import tpu as pltpu
from jax.sharding import PartitionSpec as P

MESH = pl.DeviceIdType.MESH
TILE = 256
SLOTS = 3


def ring_map(place, n):
    if n % 4:
        return place
    return place + ((place % 4) // 2) * (1 - 2 * (place % 2))


def plane_at(q, c, m):
    near = jnp.minimum(c, m - 1 - c)
    away = jnp.where(2 * c < m, 1, -1)
    both = away * ((q + 1) // 2) if q % 2 else -away * (q // 2)
    return c + jnp.where(q <= 2 * near, both, away * (q - near))


def plane_dot(n, m, rows, every, held, plane, cols):
    chunk = held.shape[2]
    side = plane * rows // chunk
    lanes = pl.ds(pl.multiple_of(plane * rows % chunk, rows), rows)
    left = [held[2 * tok + side, :, lanes] for tok in range(n)]
    right = [every[pl.ds(pl.multiple_of((tok * m + plane) * rows, rows), rows), cols] for tok in range(n)]
    return jnp.dot(
        jnp.concatenate(left, axis=1), jnp.concatenate(right, axis=0),
        preferred_element_type=jnp.float32)


def finish(n, m, every, held, acc, out, tile, sem):
    rows = every.shape[0] // (n * m)
    slots, _, width = tile.shape
    steps = acc.shape[1] // width
    plane = plane_at(m - 1, lax.axis_index("col"), m)

    def leave(i):
        cols = pl.ds(pl.multiple_of(i * width, width), width)
        return pltpu.make_async_copy(tile.at[i % slots], out.at[0, :, cols], sem.at[i % slots])

    @pl.loop(0, steps)
    def _(i):
        @pl.when(i >= slots)
        def _():
            leave(i - slots).wait()

        cols = pl.ds(pl.multiple_of(i * width, width), width)
        tile[i % slots] = acc[:, cols] + plane_dot(n, m, rows, every, held, plane, cols)
        leave(i).start()

    @pl.loop(max(0, steps - slots), steps)
    def _(i):
        leave(i).wait()


def fused(n, m, acts, grads, every, held, acc,
          local_sem, zsend, zrecv, rsend, rrecv, gsend, grecv, psend):
    k, r, c = lax.axis_index("tok"), lax.axis_index("row"), lax.axis_index("col")
    place = ring_map(k, n)
    rows, wide = acts.shape
    quarter = wide // 4
    chunk = grads.shape[2]
    up, down = c + 1 < m, c > 0
    reach = ((n // 2, n - 1 - n // 2), (n - 1 - n // 2, n // 2))
    hops = n // 2

    def member(offset):
        return ring_map((place + offset + 2 * n) % n, n)

    barrier = pltpu.get_barrier_semaphore()
    for j in range(1, n):
        pl.semaphore_signal(barrier, inc=1, device_id={"tok": (k + j) % n}, device_id_type=MESH)
    pl.semaphore_signal(barrier, inc=1, device_id={"row": 1 - r}, device_id_type=MESH)

    @pl.when(up)
    def _():
        pl.semaphore_signal(barrier, inc=1, device_id={"col": c + 1}, device_id_type=MESH)

    @pl.when(down)
    def _():
        pl.semaphore_signal(barrier, inc=1, device_id={"col": c - 1}, device_id_type=MESH)

    def span(tok, col):
        return pl.ds(pl.multiple_of((tok * m + col) * rows, rows), rows)

    def at_slot(tok, side):
        return held.at[tok * 2 + side]

    own = every.at[span(k, c), :]
    enter = pltpu.make_async_copy(acts, own, local_sem.at[0])
    enter_g = pltpu.make_async_copy(grads.at[k], at_slot(k, r), local_sem.at[1])

    @pl.when(up & down)
    def _():
        pl.semaphore_wait(barrier, n + 2)

    @pl.when(jnp.logical_not(up & down))
    def _():
        pl.semaphore_wait(barrier, n + 1)

    def z_copy(item, tok, col, way, fresh=False):
        begin = 0 if isinstance(item, int) and item == 0 else 2 * quarter
        cols = pl.ds(begin, 2 * quarter)
        where = every.at[span(tok, col), cols]
        return pltpu.make_async_remote_copy(
            acts.at[:, cols] if fresh else where, where,
            zsend.at[way, item, col], zrecv.at[item, col],
            device_id={"col": c + 1 - 2 * way}, device_id_type=MESH)

    def z_start(item, tok, fresh=False):
        @pl.when(up)
        def _():
            z_copy(item, tok, c, 0, fresh).start()

        @pl.when(down)
        def _():
            z_copy(item, tok, c, 1, fresh).start()

    def z_round(s, item, tok):
        below, above = c - 1 - s, c + 1 + s

        @pl.when(below >= 0)
        def _():
            z_copy(item, tok, below, 0).wait_recv()

            @pl.when(up)
            def _():
                z_copy(item, tok, below, 0).start()

        @pl.when(above < m)
        def _():
            z_copy(item, tok, above, 1).wait_recv()

            @pl.when(down)
            def _():
                z_copy(item, tok, above, 1).start()

    def ring_copy(line, col, offset, half, way, fresh=False):
        begin = 2 * quarter if isinstance(line, int) and line == m else 0
        cols = pl.ds(begin + half * quarter, quarter)
        tok = member(offset)
        where = every.at[span(tok, col), cols]
        return pltpu.make_async_remote_copy(
            acts.at[:, cols] if fresh else where, where,
            rsend.at[way, line, tok, half], rrecv.at[line, tok, half],
            device_id={"tok": member(1 - 2 * way)}, device_id_type=MESH)

    def ring_start(line, col, fresh=False):
        for half in range(2):
            for way in range(2):
                which = half if way == 0 else 1 - half
                if reach[which][way] >= 1:
                    ring_copy(line, col, 0, which, way, fresh).start()

    def ring_step(line, col, t):
        for half in range(2):
            for way in range(2):
                which = half if way == 0 else 1 - half
                if reach[which][way] >= t:
                    offset = -t if way == 0 else t
                    ring_copy(line, col, offset, which, way).wait_recv()
                    if reach[which][way] > t:
                        ring_copy(line, col, offset, which, way).start()

    def ring_sent(line, col):
        for half in range(2):
            for way in range(2):
                for t in range(reach[half][way]):
                    ring_copy(line, col, -t if way == 0 else t, half, way).wait_send()

    def at_distance(d, do):
        @pl.when(c - d >= 0)
        def _():
            do(c - d, c - d)

        @pl.when((c + d < m) & (d > 0))
        def _():
            do(c + d, c + d)

    def g_send(j):
        to = (k + j) % n
        return pltpu.make_async_remote_copy(
            grads.at[to], at_slot(k, r), gsend.at[j], grecv.at[k, r],
            device_id={"tok": to}, device_id_type=MESH)

    def g_recv(tok):
        where = at_slot(tok, r)
        return pltpu.make_async_remote_copy(
            where, where, gsend.at[0], grecv.at[tok, r],
            device_id={"row": 1 - r}, device_id_type=MESH)

    def partner(tok, side, fresh=False):
        where = at_slot(tok, side)
        return pltpu.make_async_remote_copy(
            grads.at[tok] if fresh else where, where, psend.at[tok], grecv.at[tok, side],
            device_id={"row": 1 - r}, device_id_type=MESH)

    ring_start(m, c, True)
    z_start(0, k, True)
    z_start(1, k, True)
    ring_start(c, c, True)
    partner(k, r, True).start()
    enter.start()
    enter_g.start()
    enter.wait()
    enter_g.wait()
    for t in range(1, hops + 1):
        ring_step(m, c, t)
        if t == 1:
            for j in sorted(range(1, n), key=lambda j: (min(j, n - j), j)):
                g_send(j).start()
        z_start(1 + (n - t), member(-t))
        if 2 * t != n:
            z_start(1 + t, member(t))

    def item_order():
        order = [0]
        for t in range(1, hops + 1):
            order.append(n - t)
            if 2 * t != n:
                order.append(t)
        return order

    def whole_round(s):
        z_round(s, 0, k)
        at_distance(s + 1, ring_start)
        for j in item_order():
            z_round(s, 1 + j, member(j))

    @pl.loop(0, m - 2)
    def _(s):
        whole_round(s)

    for j in sorted(range(1, n), key=lambda j: (min(j, n - j), j)):
        tok = (k + n - j) % n
        g_recv(tok).wait_recv()
        partner(tok, r).start()

    @pl.loop(0, m - 1)
    def _(d):
        at_distance(d, functools.partial(ring_step, t=1))

    @pl.loop(0, n)
    def _(j):
        partner((k + j) % n, 1 - r).wait_recv()

    tiles = wide // TILE

    def multiply(q, half):
        plane = plane_at(q, c, m)

        @pl.loop(half * tiles // 2, (half + 1) * tiles // 2)
        def _(i):
            cols = pl.ds(pl.multiple_of(i * TILE, TILE), TILE)
            part = plane_dot(n, m, rows, every, held, plane, cols)
            acc[:, cols] = part if q == 0 else acc[:, cols] + part

    def last_hops(d):
        for t in range(2, hops + 1):
            at_distance(d, functools.partial(ring_step, t=t))

    multiply(0, 1)
    z_round(m - 2, 0, k)
    at_distance(m - 1, ring_start)
    if m > 2:
        multiply(1, 1)
    at_distance(m - 1, functools.partial(ring_step, t=1))
    for place_in_order, j in enumerate(item_order()):
        z_round(m - 2, 1 + j, member(j))
        if place_in_order == 0:
            for q in range(2, m - 1):
                multiply(q, 1)
        if place_in_order < m - 1:
            last_hops(place_in_order)
            multiply(place_in_order, 0)
    for q in range(n, m - 1):
        last_hops(q)
        multiply(q, 0)
    last_hops(m - 1)

    for j in range(1, n):
        g_send(j).wait_send()

    @pl.loop(0, n)
    def _(j):
        partner(j, r).wait_send()

    ring_sent(m, c)

    @pl.loop(0, m)
    def _(d):
        at_distance(d, ring_sent)

    def z_sent(item, tok):
        @pl.loop(0, m)
        def _(col):
            @pl.when((col <= c) & up)
            def _():
                z_copy(item, tok, col, 0).wait_send()

            @pl.when((col >= c) & down)
            def _():
                z_copy(item, tok, col, 1).wait_send()

    z_sent(0, k)
    for j in range(n):
        z_sent(1 + j, member(j))


def kernel(n, m, acts, grads, every, held, stage, stage_g,
           local_sem, zsend, zrecv, rsend, rrecv, gsend, grecv, psend):
    k, r, c = lax.axis_index("tok"), lax.axis_index("row"), lax.axis_index("col")
    place = ring_map(k, n)
    rows, wide = acts.shape
    quarter = wide // 4
    chunk = grads.shape[2]
    up, down = c + 1 < m, c > 0
    reach = ((n // 2, n - 1 - n // 2), (n - 1 - n // 2, n // 2))
    hops = n // 2

    def member(offset):
        return ring_map((place + offset + 2 * n) % n, n)

    barrier = pltpu.get_barrier_semaphore()
    for j in range(1, n):
        pl.semaphore_signal(barrier, inc=1, device_id={"tok": (k + j) % n}, device_id_type=MESH)
    pl.semaphore_signal(barrier, inc=1, device_id={"row": 1 - r}, device_id_type=MESH)

    @pl.when(up)
    def _():
        pl.semaphore_signal(barrier, inc=1, device_id={"col": c + 1}, device_id_type=MESH)

    @pl.when(down)
    def _():
        pl.semaphore_signal(barrier, inc=1, device_id={"col": c - 1}, device_id_type=MESH)

    def span(tok, col):
        return pl.ds(pl.multiple_of((tok * m + col) * rows, rows), rows)

    def at_slot(tok, side):
        return held.at[:, pl.ds(pl.multiple_of((tok * 2 + side) * chunk, chunk), chunk)]

    own = every.at[span(k, c), :]
    enter = pltpu.make_async_copy(acts, stage, local_sem.at[0])
    enter_g = pltpu.make_async_copy(grads.at[k], stage_g, local_sem.at[1])
    leave = pltpu.make_async_copy(stage, own, local_sem.at[2])
    leave_g = pltpu.make_async_copy(stage_g, at_slot(k, r), local_sem.at[3])

    @pl.when(up & down)
    def _():
        pl.semaphore_wait(barrier, n + 2)

    @pl.when(jnp.logical_not(up & down))
    def _():
        pl.semaphore_wait(barrier, n + 1)

    def z_copy(item, tok, col, way, fresh=False):
        begin = 0 if isinstance(item, int) and item == 0 else 2 * quarter
        cols = pl.ds(begin, 2 * quarter)
        where = every.at[span(tok, col), cols]
        return pltpu.make_async_remote_copy(
            acts.at[:, cols] if fresh else where, where,
            zsend.at[way, item, col], zrecv.at[item, col],
            device_id={"col": c + 1 - 2 * way}, device_id_type=MESH)

    def z_start(item, tok, fresh=False):
        @pl.when(up)
        def _():
            z_copy(item, tok, c, 0, fresh).start()

        @pl.when(down)
        def _():
            z_copy(item, tok, c, 1, fresh).start()

    def z_round(s, item, tok):
        below, above = c - 1 - s, c + 1 + s

        @pl.when(below >= 0)
        def _():
            z_copy(item, tok, below, 0).wait_recv()

            @pl.when(up)
            def _():
                z_copy(item, tok, below, 0).start()

        @pl.when(above < m)
        def _():
            z_copy(item, tok, above, 1).wait_recv()

            @pl.when(down)
            def _():
                z_copy(item, tok, above, 1).start()

    def ring_copy(line, col, offset, half, way, fresh=False):
        begin = 2 * quarter if isinstance(line, int) and line == m else 0
        cols = pl.ds(begin + half * quarter, quarter)
        tok = member(offset)
        where = every.at[span(tok, col), cols]
        return pltpu.make_async_remote_copy(
            acts.at[:, cols] if fresh else where, where,
            rsend.at[way, line, tok, half], rrecv.at[line, tok, half],
            device_id={"tok": member(1 - 2 * way)}, device_id_type=MESH)

    def ring_start(line, col, fresh=False):
        for half in range(2):
            for way in range(2):
                which = half if way == 0 else 1 - half
                if reach[which][way] >= 1:
                    ring_copy(line, col, 0, which, way, fresh).start()

    def ring_step(line, col, t):
        for half in range(2):
            for way in range(2):
                which = half if way == 0 else 1 - half
                if reach[which][way] >= t:
                    offset = -t if way == 0 else t
                    ring_copy(line, col, offset, which, way).wait_recv()
                    if reach[which][way] > t:
                        ring_copy(line, col, offset, which, way).start()

    def ring_sent(line, col):
        for half in range(2):
            for way in range(2):
                for t in range(reach[half][way]):
                    ring_copy(line, col, -t if way == 0 else t, half, way).wait_send()

    def at_distance(d, do):
        @pl.when(c - d >= 0)
        def _():
            do(c - d, c - d)

        @pl.when((c + d < m) & (d > 0))
        def _():
            do(c + d, c + d)

    def g_send(j):
        to = (k + j) % n
        return pltpu.make_async_remote_copy(
            grads.at[to], at_slot(k, r), gsend.at[j], grecv.at[k, r],
            device_id={"tok": to}, device_id_type=MESH)

    def g_recv(tok):
        where = at_slot(tok, r)
        return pltpu.make_async_remote_copy(
            where, where, gsend.at[0], grecv.at[tok, r],
            device_id={"row": 1 - r}, device_id_type=MESH)

    def partner(tok, side, fresh=False):
        where = at_slot(tok, side)
        return pltpu.make_async_remote_copy(
            grads.at[tok] if fresh else where, where, psend.at[tok], grecv.at[tok, side],
            device_id={"row": 1 - r}, device_id_type=MESH)

    ring_start(m, c, True)
    z_start(0, k, True)
    z_start(1, k, True)
    ring_start(c, c, True)
    partner(k, r, True).start()
    enter.start()
    enter_g.start()
    enter.wait()
    leave.start()
    enter_g.wait()
    leave_g.start()
    for t in range(1, hops + 1):
        ring_step(m, c, t)
        if t == 1:
            for j in sorted(range(1, n), key=lambda j: (min(j, n - j), j)):
                g_send(j).start()
        z_start(1 + (n - t), member(-t))
        if 2 * t != n:
            z_start(1 + t, member(t))

    def item_order():
        order = [0]
        for t in range(1, hops + 1):
            order.append(n - t)
            if 2 * t != n:
                order.append(t)
        return order

    def whole_round(s):
        z_round(s, 0, k)
        at_distance(s + 1, ring_start)
        for j in item_order():
            z_round(s, 1 + j, member(j))

    @pl.loop(0, m - 2)
    def _(s):
        whole_round(s)

    for j in sorted(range(1, n), key=lambda j: (min(j, n - j), j)):
        tok = (k + n - j) % n
        g_recv(tok).wait_recv()
        partner(tok, r).start()

    @pl.loop(0, m - 1)
    def _(d):
        at_distance(d, functools.partial(ring_step, t=1))

    @pl.loop(0, n)
    def _(j):
        partner((k + j) % n, 1 - r).wait_recv()

    z_round(m - 2, 0, k)
    at_distance(m - 1, ring_start)
    at_distance(m - 1, functools.partial(ring_step, t=1))
    for j in item_order():
        z_round(m - 2, 1 + j, member(j))
    for t in range(2, hops + 1):
        @pl.loop(0, m)
        def _(d):
            at_distance(d, functools.partial(ring_step, t=t))

    for j in range(1, n):
        g_send(j).wait_send()

    @pl.loop(0, n)
    def _(j):
        partner(j, r).wait_send()

    ring_sent(m, c)

    @pl.loop(0, m)
    def _(d):
        at_distance(d, ring_sent)

    def z_sent(item, tok):
        @pl.loop(0, m)
        def _(col):
            @pl.when((col <= c) & up)
            def _():
                z_copy(item, tok, col, 0).wait_send()

            @pl.when((col >= c) & down)
            def _():
                z_copy(item, tok, col, 1).wait_send()

    z_sent(0, k)
    for j in range(n):
        z_sent(1 + j, member(j))
    leave.wait()
    leave_g.wait()


def plain_body(n, m, activations, grads_t):
    _, units, chunk = grads_t.shape
    rows, wide = activations.shape
    tokens = rows * n * m
    dma = pltpu.SemaphoreType.DMA
    every, held = pl.pallas_call(
        functools.partial(kernel, n, m),
        out_shape=(
            jax.ShapeDtypeStruct((tokens, wide), jnp.bfloat16),
            jax.ShapeDtypeStruct((units, n * 2 * chunk), jnp.bfloat16),
        ),
        in_specs=[pl.BlockSpec(memory_space=pl.ANY)] * 2,
        out_specs=[pl.BlockSpec(memory_space=pl.ANY)] * 2,
        scratch_shapes=[
            pltpu.VMEM((rows, wide), jnp.bfloat16),
            pltpu.VMEM((units, chunk), jnp.bfloat16),
            dma((4,)),
            dma((2, n + 1, m)),
            dma((n + 1, m)),
            dma((2, m + 1, n, 2)),
            dma((m + 1, n, 2)),
            dma((n,)),
            dma((n, 2)),
            dma((n,)),
        ],
        compiler_params=pltpu.CompilerParams(
            collective_id=0, has_side_effects=True, vmem_limit_bytes=60 * 2**20),
    )(activations, grads_t)
    return jnp.dot(held, every, preferred_element_type=jnp.float32)[None]


def semaphores(n, m):
    dma = pltpu.SemaphoreType.DMA
    return [
        dma((4,)),
        dma((2, n + 1, m)),
        dma((n + 1, m)),
        dma((2, m + 1, n, 2)),
        dma((m + 1, n, 2)),
        dma((n,)),
        dma((n, 2)),
        dma((n,)),
    ]


def fused_body(n, m, activations, grads_t):
    _, units, chunk = grads_t.shape
    rows, wide = activations.shape
    every, held, acc = pl.pallas_call(
        functools.partial(fused, n, m),
        out_shape=(
            pltpu.VMEM((rows * n * m, wide), jnp.bfloat16),
            pltpu.VMEM((n * 2, units, chunk), jnp.bfloat16),
            pltpu.VMEM((units, wide), jnp.float32),
        ),
        in_specs=[pl.BlockSpec(memory_space=pl.ANY)] * 2,
        out_specs=[pl.BlockSpec(memory_space=pltpu.VMEM)] * 3,
        scratch_shapes=semaphores(n, m),
        compiler_params=pltpu.CompilerParams(
            collective_id=0, has_side_effects=True, vmem_limit_bytes=26 * 2**20),
    )(activations, grads_t)
    return pl.pallas_call(
        functools.partial(finish, n, m),
        out_shape=jax.ShapeDtypeStruct((1, units, wide), jnp.float32),
        in_specs=[pl.BlockSpec(memory_space=pltpu.VMEM)] * 3,
        out_specs=pl.BlockSpec(memory_space=pl.ANY),
        scratch_shapes=[
            pltpu.VMEM((SLOTS, units, TILE), jnp.float32),
            pltpu.SemaphoreType.DMA((SLOTS,)),
        ],
        compiler_params=pltpu.CompilerParams(vmem_limit_bytes=20 * 2**20),
    )(every, held, acc)


def body(n, m, activations, grads_t):
    _, units, chunk = grads_t.shape
    rows, wide = activations.shape
    resident = 2 * n * units * chunk * 2 + rows * n * m * wide * 2 + units * wide * 4
    fits = rows % 128 == 0 and chunk % rows == 0 and wide % (2 * TILE) == 0
    if fits and m > 1 and resident <= 32 * 2**20:
        return fused_body(n, m, activations, grads_t)
    return plain_body(n, m, activations, grads_t)


def solution(mesh):
    return jax.shard_map(
        functools.partial(body, mesh.shape["tok"], mesh.shape["col"]),
        mesh=mesh,
        in_specs=(P(("tok", "col"), "row"), P(None, "col", ("tok", "row"))),
        out_specs=P("tok", "col", "row"),
        check_vma=False,
    )
```

```python
import functools

import jax
import jax.numpy as jnp
from jax import lax
from jax.experimental import pallas as pl
from jax.experimental.pallas import tpu as pltpu
from jax.sharding import PartitionSpec as P

MESH = pl.DeviceIdType.MESH
TILE = 256
SLOTS = 3


def ring_map(place, n):
    if n % 4:
        return place
    return place + ((place % 4) // 2) * (1 - 2 * (place % 2))


def plane_at(q, c, m):
    near = jnp.minimum(c, m - 1 - c)
    away = jnp.where(2 * c < m, 1, -1)
    both = away * ((q + 1) // 2) if q % 2 else -away * (q // 2)
    return c + jnp.where(q <= 2 * near, both, away * (q - near))


def plane_dot(n, m, rows, every, held, plane, cols):
    chunk = held.shape[2]
    side = plane * rows // chunk
    lanes = pl.ds(pl.multiple_of(plane * rows % chunk, rows), rows)
    left = [held[2 * tok + side, :, lanes] for tok in range(n)]
    right = [every[pl.ds(pl.multiple_of((tok * m + plane) * rows, rows), rows), cols] for tok in range(n)]
    return jnp.dot(
        jnp.concatenate(left, axis=1), jnp.concatenate(right, axis=0),
        preferred_element_type=jnp.float32)


def finish(n, m, every, held, acc, out, tile, sem):
    rows = every.shape[0] // (n * m)
    slots, _, width = tile.shape
    steps = acc.shape[1] // width
    plane = plane_at(m - 1, lax.axis_index("col"), m)

    def leave(i):
        cols = pl.ds(pl.multiple_of(i * width, width), width)
        return pltpu.make_async_copy(tile.at[i % slots], out.at[0, :, cols], sem.at[i % slots])

    @pl.loop(0, steps)
    def _(i):
        @pl.when(i >= slots)
        def _():
            leave(i - slots).wait()

        cols = pl.ds(pl.multiple_of(i * width, width), width)
        tile[i % slots] = acc[:, cols] + plane_dot(n, m, rows, every, held, plane, cols)
        leave(i).start()

    @pl.loop(max(0, steps - slots), steps)
    def _(i):
        leave(i).wait()


def fused(n, m, acts, grads, every, held, acc,
          local_sem, zsend, zrecv, rsend, rrecv, gsend, grecv, psend):
    k, r, c = lax.axis_index("tok"), lax.axis_index("row"), lax.axis_index("col")
    place = ring_map(k, n)
    rows, wide = acts.shape
    units = grads.shape[1]
    quarter = wide // 4
    chunk = grads.shape[2]
    up, down = c + 1 < m, c > 0
    reach = ((n // 2, n - 1 - n // 2), (n - 1 - n // 2, n // 2))
    hops = n // 2

    def member(offset):
        return ring_map((place + offset + 2 * n) % n, n)

    barrier = pltpu.get_barrier_semaphore()
    for j in range(1, n):
        pl.semaphore_signal(barrier, inc=1, device_id={"tok": (k + j) % n}, device_id_type=MESH)
    pl.semaphore_signal(barrier, inc=1, device_id={"row": 1 - r}, device_id_type=MESH)

    @pl.when(up)
    def _():
        pl.semaphore_signal(barrier, inc=1, device_id={"col": c + 1}, device_id_type=MESH)

    @pl.when(down)
    def _():
        pl.semaphore_signal(barrier, inc=1, device_id={"col": c - 1}, device_id_type=MESH)

    def span(tok, col):
        return pl.ds(pl.multiple_of((tok * m + col) * rows, rows), rows)

    def at_slot(tok, side):
        return held.at[tok * 2 + side]

    own = every.at[span(k, c), :]
    enter = pltpu.make_async_copy(acts, own, local_sem.at[0])
    enter_g = pltpu.make_async_copy(grads.at[k], at_slot(k, r), local_sem.at[1])

    @pl.when(up & down)
    def _():
        pl.semaphore_wait(barrier, n + 2)

    @pl.when(jnp.logical_not(up & down))
    def _():
        pl.semaphore_wait(barrier, n + 1)

    def z_copy(item, tok, col, way, fresh=False):
        begin = 0 if isinstance(item, int) and item == 0 else 2 * quarter
        cols = pl.ds(begin, 2 * quarter)
        where = every.at[span(tok, col), cols]
        return pltpu.make_async_remote_copy(
            acts.at[:, cols] if fresh else where, where,
            zsend.at[way, item, col], zrecv.at[item, col],
            device_id={"col": c + 1 - 2 * way}, device_id_type=MESH)

    def z_start(item, tok, fresh=False):
        @pl.when(up)
        def _():
            z_copy(item, tok, c, 0, fresh).start()

        @pl.when(down)
        def _():
            z_copy(item, tok, c, 1, fresh).start()

    def z_round(s, item, tok):
        below, above = c - 1 - s, c + 1 + s

        @pl.when(below >= 0)
        def _():
            z_copy(item, tok, below, 0).wait_recv()

            @pl.when(up)
            def _():
                z_copy(item, tok, below, 0).start()

        @pl.when(above < m)
        def _():
            z_copy(item, tok, above, 1).wait_recv()

            @pl.when(down)
            def _():
                z_copy(item, tok, above, 1).start()

    def ring_copy(line, col, offset, half, way, fresh=False):
        begin = 2 * quarter if isinstance(line, int) and line == m else 0
        cols = pl.ds(begin + half * quarter, quarter)
        tok = member(offset)
        where = every.at[span(tok, col), cols]
        return pltpu.make_async_remote_copy(
            acts.at[:, cols] if fresh else where, where,
            rsend.at[way, line, tok, half], rrecv.at[line, tok, half],
            device_id={"tok": member(1 - 2 * way)}, device_id_type=MESH)

    def ring_start(line, col, fresh=False):
        for half in range(2):
            for way in range(2):
                which = half if way == 0 else 1 - half
                if reach[which][way] >= 1:
                    ring_copy(line, col, 0, which, way, fresh).start()

    def ring_step(line, col, t):
        for half in range(2):
            for way in range(2):
                which = half if way == 0 else 1 - half
                if reach[which][way] >= t:
                    offset = -t if way == 0 else t
                    ring_copy(line, col, offset, which, way).wait_recv()
                    if reach[which][way] > t:
                        ring_copy(line, col, offset, which, way).start()

    def ring_sent(line, col):
        for half in range(2):
            for way in range(2):
                for t in range(reach[half][way]):
                    ring_copy(line, col, -t if way == 0 else t, half, way).wait_send()

    def at_distance(d, do):
        @pl.when(c - d >= 0)
        def _():
            do(c - d, c - d)

        @pl.when((c + d < m) & (d > 0))
        def _():
            do(c + d, c + d)

    pieces = max(p for p in range(1, 9) if units % (8 * p) == 0)
    others = sorted(range(1, n), key=lambda j: (min(j, n - j), j))

    def g_send(j, piece=None):
        to = (k + j) % n
        part = (pl.ds(0, units) if piece is None
                else pl.ds(piece * (units // pieces), units // pieces))
        return pltpu.make_async_remote_copy(
            grads.at[to, part], at_slot(k, r).at[part], gsend.at[j], grecv.at[k, r],
            device_id={"tok": to}, device_id_type=MESH)

    def g_start(piece):
        for j in others:
            g_send(j, piece).start()

    def g_recv(tok):
        where = at_slot(tok, r)
        return pltpu.make_async_remote_copy(
            where, where, gsend.at[0], grecv.at[tok, r],
            device_id={"row": 1 - r}, device_id_type=MESH)

    def partner(tok, side, fresh=False):
        where = at_slot(tok, side)
        return pltpu.make_async_remote_copy(
            grads.at[tok] if fresh else where, where, psend.at[tok], grecv.at[tok, side],
            device_id={"row": 1 - r}, device_id_type=MESH)

    tiles = wide // TILE

    def multiply(q, half):
        plane = plane_at(q, c, m)

        @pl.loop(half * tiles // 2, (half + 1) * tiles // 2)
        def _(i):
            cols = pl.ds(pl.multiple_of(i * TILE, TILE), TILE)
            part = plane_dot(n, m, rows, every, held, plane, cols)
            acc[:, cols] = part if (q, half) in first else acc[:, cols] + part

    first = ((0, 0), (0, 1))

    def line_start(d):
        at_distance(d, ring_start)

    def line_step(d, t):
        at_distance(d, functools.partial(ring_step, t=t))

    def pass_grads():
        for j in others:
            tok = (k + n - j) % n
            g_recv(tok).wait_recv()
            partner(tok, r).start()

    def all_grads():
        for j in range(n):
            partner((k + j) % n, 1 - r).wait_recv()

    per_round = n + 1
    plan = []
    for p in range(2, pieces):
        plan.append((p - 1, 1, functools.partial(g_start, p)))
    passed = pieces + 1
    plan.append((passed, 2, pass_grads))
    plan.append((passed + 1, 2, all_grads))
    for d in range(m):
        begin = max(pieces - 1 + d, (d - 1) * per_round)
        plan.append((begin, 1, functools.partial(line_start, d)))
        plan.append((begin + 3, 0, functools.partial(line_step, d, 1)))
        for t in range(2, hops + 1):
            plan.append((begin + 1 + 2 * t, 0, functools.partial(line_step, d, t)))
        if d < m - 1:
            there = max(passed + 1 + d, d * per_round - 1)
            plan.append((there, 3, functools.partial(multiply, d, 1)))
            there = max(there, begin + 1 + 2 * hops)
            plan.append((there, 4, functools.partial(multiply, d, 0)))
    plan.sort(key=lambda entry: entry[:2])

    ring_start(m, c, True)
    z_start(0, k, True)
    z_start(1, k, True)
    partner(k, r, True).start()
    enter.start()
    enter_g.start()
    enter.wait()
    enter_g.wait()
    for t in range(1, hops + 1):
        ring_step(m, c, t)
        if t <= min(2, pieces):
            g_start(t - 1)
        z_start(1 + (n - t), member(-t))
        if 2 * t != n:
            z_start(1 + t, member(t))
    for p in range(hops, min(2, pieces)):
        g_start(p)

    items = [(0, k)]
    for t in range(1, hops + 1):
        items.append((1 + n - t, member(-t)))
        if 2 * t != n:
            items.append((1 + t, member(t)))
    items.insert(1, (1, k))
    for slot in range((m - 1) * per_round):
        z_round(slot // per_round, *items[slot % per_round])
        while plan and plan[0][0] <= slot:
            plan.pop(0)[2]()
    for _, _, act in plan:
        act()

    for j in range(1, n):
        g_send(j).wait_send()

    @pl.loop(0, n)
    def _(j):
        partner(j, r).wait_send()

    ring_sent(m, c)

    @pl.loop(0, m)
    def _(d):
        at_distance(d, ring_sent)

    def z_sent(item, tok):
        @pl.loop(0, m)
        def _(col):
            @pl.when((col <= c) & up)
            def _():
                z_copy(item, tok, col, 0).wait_send()

            @pl.when((col >= c) & down)
            def _():
                z_copy(item, tok, col, 1).wait_send()

    z_sent(0, k)
    for j in range(n):
        z_sent(1 + j, member(j))


def kernel(n, m, acts, grads, every, held, stage, stage_g,
           local_sem, zsend, zrecv, rsend, rrecv, gsend, grecv, psend):
    k, r, c = lax.axis_index("tok"), lax.axis_index("row"), lax.axis_index("col")
    place = ring_map(k, n)
    rows, wide = acts.shape
    quarter = wide // 4
    chunk = grads.shape[2]
    up, down = c + 1 < m, c > 0
    reach = ((n // 2, n - 1 - n // 2), (n - 1 - n // 2, n // 2))
    hops = n // 2

    def member(offset):
        return ring_map((place + offset + 2 * n) % n, n)

    barrier = pltpu.get_barrier_semaphore()
    for j in range(1, n):
        pl.semaphore_signal(barrier, inc=1, device_id={"tok": (k + j) % n}, device_id_type=MESH)
    pl.semaphore_signal(barrier, inc=1, device_id={"row": 1 - r}, device_id_type=MESH)

    @pl.when(up)
    def _():
        pl.semaphore_signal(barrier, inc=1, device_id={"col": c + 1}, device_id_type=MESH)

    @pl.when(down)
    def _():
        pl.semaphore_signal(barrier, inc=1, device_id={"col": c - 1}, device_id_type=MESH)

    def span(tok, col):
        return pl.ds(pl.multiple_of((tok * m + col) * rows, rows), rows)

    def at_slot(tok, side):
        return held.at[:, pl.ds(pl.multiple_of((tok * 2 + side) * chunk, chunk), chunk)]

    own = every.at[span(k, c), :]
    enter = pltpu.make_async_copy(acts, stage, local_sem.at[0])
    enter_g = pltpu.make_async_copy(grads.at[k], stage_g, local_sem.at[1])
    leave = pltpu.make_async_copy(stage, own, local_sem.at[2])
    leave_g = pltpu.make_async_copy(stage_g, at_slot(k, r), local_sem.at[3])

    @pl.when(up & down)
    def _():
        pl.semaphore_wait(barrier, n + 2)

    @pl.when(jnp.logical_not(up & down))
    def _():
        pl.semaphore_wait(barrier, n + 1)

    def z_copy(item, tok, col, way, fresh=False):
        begin = 0 if isinstance(item, int) and item == 0 else 2 * quarter
        cols = pl.ds(begin, 2 * quarter)
        where = every.at[span(tok, col), cols]
        return pltpu.make_async_remote_copy(
            acts.at[:, cols] if fresh else where, where,
            zsend.at[way, item, col], zrecv.at[item, col],
            device_id={"col": c + 1 - 2 * way}, device_id_type=MESH)

    def z_start(item, tok, fresh=False):
        @pl.when(up)
        def _():
            z_copy(item, tok, c, 0, fresh).start()

        @pl.when(down)
        def _():
            z_copy(item, tok, c, 1, fresh).start()

    def z_round(s, item, tok):
        below, above = c - 1 - s, c + 1 + s

        @pl.when(below >= 0)
        def _():
            z_copy(item, tok, below, 0).wait_recv()

            @pl.when(up)
            def _():
                z_copy(item, tok, below, 0).start()

        @pl.when(above < m)
        def _():
            z_copy(item, tok, above, 1).wait_recv()

            @pl.when(down)
            def _():
                z_copy(item, tok, above, 1).start()

    def ring_copy(line, col, offset, half, way, fresh=False):
        begin = 2 * quarter if isinstance(line, int) and line == m else 0
        cols = pl.ds(begin + half * quarter, quarter)
        tok = member(offset)
        where = every.at[span(tok, col), cols]
        return pltpu.make_async_remote_copy(
            acts.at[:, cols] if fresh else where, where,
            rsend.at[way, line, tok, half], rrecv.at[line, tok, half],
            device_id={"tok": member(1 - 2 * way)}, device_id_type=MESH)

    def ring_start(line, col, fresh=False):
        for half in range(2):
            for way in range(2):
                which = half if way == 0 else 1 - half
                if reach[which][way] >= 1:
                    ring_copy(line, col, 0, which, way, fresh).start()

    def ring_step(line, col, t):
        for half in range(2):
            for way in range(2):
                which = half if way == 0 else 1 - half
                if reach[which][way] >= t:
                    offset = -t if way == 0 else t
                    ring_copy(line, col, offset, which, way).wait_recv()
                    if reach[which][way] > t:
                        ring_copy(line, col, offset, which, way).start()

    def ring_sent(line, col):
        for half in range(2):
            for way in range(2):
                for t in range(reach[half][way]):
                    ring_copy(line, col, -t if way == 0 else t, half, way).wait_send()

    def at_distance(d, do):
        @pl.when(c - d >= 0)
        def _():
            do(c - d, c - d)

        @pl.when((c + d < m) & (d > 0))
        def _():
            do(c + d, c + d)

    def g_send(j):
        to = (k + j) % n
        return pltpu.make_async_remote_copy(
            grads.at[to], at_slot(k, r), gsend.at[j], grecv.at[k, r],
            device_id={"tok": to}, device_id_type=MESH)

    def g_recv(tok):
        where = at_slot(tok, r)
        return pltpu.make_async_remote_copy(
            where, where, gsend.at[0], grecv.at[tok, r],
            device_id={"row": 1 - r}, device_id_type=MESH)

    def partner(tok, side, fresh=False):
        where = at_slot(tok, side)
        return pltpu.make_async_remote_copy(
            grads.at[tok] if fresh else where, where, psend.at[tok], grecv.at[tok, side],
            device_id={"row": 1 - r}, device_id_type=MESH)

    ring_start(m, c, True)
    z_start(0, k, True)
    z_start(1, k, True)
    ring_start(c, c, True)
    partner(k, r, True).start()
    enter.start()
    enter_g.start()
    enter.wait()
    leave.start()
    enter_g.wait()
    leave_g.start()
    for t in range(1, hops + 1):
        ring_step(m, c, t)
        if t == 1:
            for j in sorted(range(1, n), key=lambda j: (min(j, n - j), j)):
                g_send(j).start()
        z_start(1 + (n - t), member(-t))
        if 2 * t != n:
            z_start(1 + t, member(t))

    def item_order():
        order = [0]
        for t in range(1, hops + 1):
            order.append(n - t)
            if 2 * t != n:
                order.append(t)
        return order

    def whole_round(s):
        z_round(s, 0, k)
        at_distance(s + 1, ring_start)
        for j in item_order():
            z_round(s, 1 + j, member(j))

    @pl.loop(0, m - 2)
    def _(s):
        whole_round(s)

    for j in sorted(range(1, n), key=lambda j: (min(j, n - j), j)):
        tok = (k + n - j) % n
        g_recv(tok).wait_recv()
        partner(tok, r).start()

    @pl.loop(0, m - 1)
    def _(d):
        at_distance(d, functools.partial(ring_step, t=1))

    @pl.loop(0, n)
    def _(j):
        partner((k + j) % n, 1 - r).wait_recv()

    z_round(m - 2, 0, k)
    at_distance(m - 1, ring_start)
    at_distance(m - 1, functools.partial(ring_step, t=1))
    for j in item_order():
        z_round(m - 2, 1 + j, member(j))
    for t in range(2, hops + 1):
        @pl.loop(0, m)
        def _(d):
            at_distance(d, functools.partial(ring_step, t=t))

    for j in range(1, n):
        g_send(j).wait_send()

    @pl.loop(0, n)
    def _(j):
        partner(j, r).wait_send()

    ring_sent(m, c)

    @pl.loop(0, m)
    def _(d):
        at_distance(d, ring_sent)

    def z_sent(item, tok):
        @pl.loop(0, m)
        def _(col):
            @pl.when((col <= c) & up)
            def _():
                z_copy(item, tok, col, 0).wait_send()

            @pl.when((col >= c) & down)
            def _():
                z_copy(item, tok, col, 1).wait_send()

    z_sent(0, k)
    for j in range(n):
        z_sent(1 + j, member(j))
    leave.wait()
    leave_g.wait()


def plain_body(n, m, activations, grads_t):
    _, units, chunk = grads_t.shape
    rows, wide = activations.shape
    tokens = rows * n * m
    dma = pltpu.SemaphoreType.DMA
    every, held = pl.pallas_call(
        functools.partial(kernel, n, m),
        out_shape=(
            jax.ShapeDtypeStruct((tokens, wide), jnp.bfloat16),
            jax.ShapeDtypeStruct((units, n * 2 * chunk), jnp.bfloat16),
        ),
        in_specs=[pl.BlockSpec(memory_space=pl.ANY)] * 2,
        out_specs=[pl.BlockSpec(memory_space=pl.ANY)] * 2,
        scratch_shapes=[
            pltpu.VMEM((rows, wide), jnp.bfloat16),
            pltpu.VMEM((units, chunk), jnp.bfloat16),
            dma((4,)),
            dma((2, n + 1, m)),
            dma((n + 1, m)),
            dma((2, m + 1, n, 2)),
            dma((m + 1, n, 2)),
            dma((n,)),
            dma((n, 2)),
            dma((n,)),
        ],
        compiler_params=pltpu.CompilerParams(
            collective_id=0, has_side_effects=True, vmem_limit_bytes=60 * 2**20),
    )(activations, grads_t)
    return jnp.dot(held, every, preferred_element_type=jnp.float32)[None]


def semaphores(n, m):
    dma = pltpu.SemaphoreType.DMA
    return [
        dma((4,)),
        dma((2, n + 1, m)),
        dma((n + 1, m)),
        dma((2, m + 1, n, 2)),
        dma((m + 1, n, 2)),
        dma((n,)),
        dma((n, 2)),
        dma((n,)),
    ]


def fused_body(n, m, activations, grads_t):
    _, units, chunk = grads_t.shape
    rows, wide = activations.shape
    every, held, acc = pl.pallas_call(
        functools.partial(fused, n, m),
        out_shape=(
            pltpu.VMEM((rows * n * m, wide), jnp.bfloat16),
            pltpu.VMEM((n * 2, units, chunk), jnp.bfloat16),
            pltpu.VMEM((units, wide), jnp.float32),
        ),
        in_specs=[pl.BlockSpec(memory_space=pl.ANY)] * 2,
        out_specs=[pl.BlockSpec(memory_space=pltpu.VMEM)] * 3,
        scratch_shapes=semaphores(n, m),
        compiler_params=pltpu.CompilerParams(
            collective_id=0, has_side_effects=True, vmem_limit_bytes=26 * 2**20),
    )(activations, grads_t)
    return pl.pallas_call(
        functools.partial(finish, n, m),
        out_shape=jax.ShapeDtypeStruct((1, units, wide), jnp.float32),
        in_specs=[pl.BlockSpec(memory_space=pltpu.VMEM)] * 3,
        out_specs=pl.BlockSpec(memory_space=pl.ANY),
        scratch_shapes=[
            pltpu.VMEM((SLOTS, units, TILE), jnp.float32),
            pltpu.SemaphoreType.DMA((SLOTS,)),
        ],
        compiler_params=pltpu.CompilerParams(vmem_limit_bytes=20 * 2**20),
    )(every, held, acc)


def body(n, m, activations, grads_t):
    _, units, chunk = grads_t.shape
    rows, wide = activations.shape
    resident = 2 * n * units * chunk * 2 + rows * n * m * wide * 2 + units * wide * 4
    fits = rows % 128 == 0 and chunk % rows == 0 and wide % (2 * TILE) == 0
    if fits and m > 1 and resident <= 32 * 2**20:
        return fused_body(n, m, activations, grads_t)
    return plain_body(n, m, activations, grads_t)


def solution(mesh):
    return jax.shard_map(
        functools.partial(body, mesh.shape["tok"], mesh.shape["col"]),
        mesh=mesh,
        in_specs=(P(("tok", "col"), "row"), P(None, "col", ("tok", "row"))),
        out_specs=P("tok", "col", "row"),
        check_vma=False,
    )
```
